32 devices in a mesh: rep: 1, dp: 32 (over x, y, z, core).
Axes of the slice: x: 2, y: 2, z: 4, core: 2. Of those that a mesh axis runs over, the one named last changes fastest.
Arguments:
- g_w_gate: bfloat16 [32, 2, 1536, 4224], P(('rep', 'dp'))
- g_w_up: bfloat16 [32, 2, 1536, 4224], P(('rep', 'dp'))
- g_w_down: bfloat16 [32, 2, 4224, 1536], P(('rep', 'dp'))
- w_gate: bfloat16 [2, 1536, 4224], replicated
- w_up: bfloat16 [2, 1536, 4224], replicated
- w_down: bfloat16 [2, 4224, 1536], replicated
- m_w_gate: float32 [2, 1536, 4224], P(None, 'dp')
- m_w_up: float32 [2, 1536, 4224], P(None, 'dp')
- m_w_down: float32 [2, 4224, 1536], P(None, 'dp')
- v_w_gate: float32 [2, 1536, 4224], P(None, 'dp')
- v_w_up: float32 [2, 1536, 4224], P(None, 'dp')
- v_w_down: float32 [2, 4224, 1536], P(None, 'dp')
Outputs:
- output 1: bfloat16 [2, 1536, 4224], P('rep')
- output 2: bfloat16 [2, 1536, 4224], P('rep')
- output 3: bfloat16 [2, 4224, 1536], P('rep')
- output 4: float32 [2, 1536, 4224], P('rep', 'dp')
- output 5: float32 [2, 1536, 4224], P('rep', 'dp')
- output 6: float32 [2, 4224, 1536], P('rep', 'dp')
- output 7: float32 [2, 1536, 4224], P('rep', 'dp')
- output 8: float32 [2, 1536, 4224], P('rep', 'dp')
- output 9: float32 [2, 4224, 1536], P('rep', 'dp')
All inputs are finite; a program needn't handle non-finite values.
Results may differ from the reference program's by a relative error of at most 0.022.
Values are sent between devices in bfloat16 or wider.
A program may use at most 2 GiB of HBM per device.

```python
import jax
import jax.numpy as jnp
from jax import lax

DEVICES = 32
D = 1536
FF = 4224
LAYERS = 2
NAMES = ("w_gate", "w_up", "w_down")
SHAPES = {"w_gate": (LAYERS, D, FF), "w_up": (LAYERS, D, FF), "w_down": (LAYERS, FF, D)}


def setup_inputs(seed: int = 0, part: int = 0) -> dict:
    kz, *keys = jax.random.split(jax.random.key(seed), 1 + 5 * len(NAMES))
    loud = 2.0 ** jax.random.uniform(kz, (), jnp.float32, -1.0, 1.0)
    drawn = {}
    for name, key, both in zip(NAMES, keys[:3], keys[3:6], strict=True):
        own = jax.random.normal(jax.random.fold_in(key, part), (DEVICES, *SHAPES[name]), jnp.float32)
        shared = jax.random.normal(jax.random.fold_in(both, part), SHAPES[name], jnp.float32)
        drawn["g_" + name] = (loud * (0.7 * shared / DEVICES + 0.7 * own * DEVICES**-0.5)).astype(jnp.bfloat16)
    for name, key in zip(NAMES, keys[6:9], strict=True):
        drawn[name] = (jax.random.normal(key, SHAPES[name], jnp.float32) * SHAPES[name][1] ** -0.5).astype(jnp.bfloat16)
    for name, key in zip(NAMES, keys[9:12], strict=True):
        drawn["m_" + name] = loud * 0.5 * jax.random.normal(key, SHAPES[name], jnp.float32)
    for name, key in zip(NAMES, keys[12:15], strict=True):
        drawn["v_" + name] = loud * loud * jax.random.uniform(key, SHAPES[name], jnp.float32, 0.5, 1.5)
    return drawn


def adamw(w, m, v, g):
    m = 0.9 * m + 0.1 * g
    v = 0.95 * v + 0.05 * g * g
    step = m * lax.rsqrt(v + 1e-8) + 0.1 * w
    return (w - 0.02 * step).astype(jnp.bfloat16), m, v


def reference(g_w_gate, g_w_up, g_w_down, w_gate, w_up, w_down, m_w_gate, m_w_up, m_w_down, v_w_gate, v_w_up, v_w_down):
    def total(terms):
        return lax.scan(lambda so_far, term: (so_far + term.astype(jnp.float32), None), jnp.zeros(terms.shape[1:], jnp.float32), terms)[0]

    gradients = [total(terms).astype(jnp.bfloat16).astype(jnp.float32) for terms in (g_w_gate, g_w_up, g_w_down)]
    new = [
        adamw(w.astype(jnp.float32), m, v, g)
        for w, m, v, g in zip((w_gate, w_up, w_down), (m_w_gate, m_w_up, m_w_down), (v_w_gate, v_w_up, v_w_down), gradients, strict=True)
    ]
    return tuple(one[which] for which in range(3) for one in new)
```

```python
import functools

import jax
import jax.numpy as jnp
from jax import lax
from jax.experimental import pallas as pl
from jax.experimental.pallas import tpu as pltpu
from jax.sharding import PartitionSpec as P

MESH = pl.DeviceIdType.MESH
F32, BF16 = jnp.float32, jnp.bfloat16
TILES = 198
T = 33
PAIRS = 3 * 2 * TILES // T // 2
EACH = PAIRS // 3
SLOTS = 4
X, Y, ZL, ZH = range(4)
WEIGHT = (8, 4, 1, 2)
ORDER = ((X, ZL, Y, ZH), (Y, ZL, X, ZH))


class Place:
    def __init__(self):
        me = lax.axis_index("dp")
        self.core = lax.rem(me, 2)
        self.chip = lax.div(me, 2)
        z = lax.rem(self.chip, 4)
        self.bit = {X: lax.div(me, 16), Y: lax.rem(lax.div(me, 8), 2), ZL: lax.rem(z, 2), ZH: lax.div(z, 2)}
        self.peer = me + 1 - 2 * self.core
        self.partner = {b: me + 2 * WEIGHT[b] * (1 - 2 * self.bit[b]) for b in range(4)}

    def greet(self):
        barrier = pltpu.get_barrier_semaphore()
        for other in (self.peer, *self.partner.values()):
            pl.semaphore_signal(barrier, inc=1, device_id={"dp": other}, device_id_type=MESH)
        pl.semaphore_wait(barrier, 5)


def when(condition):
    return pl.when(condition)


def send(src, dst, sems, at, device):
    send_sem, recv_sem = sems
    return pltpu.make_async_remote_copy(
        src_ref=src, dst_ref=dst, send_sem=send_sem.at[at], recv_sem=recv_sem.at[at], device_id={"dp": device}, device_id_type=MESH
    )


def for_chunk(i, colour, core, act):
    k = 2 * lax.rem(i, EACH) + colour
    per = TILES // T
    for which in range(3):

        @pl.when(lax.div(i, EACH) == which)
        def _():
            if which < 2:
                act(which, lax.div(k, per), lax.rem(k, per) * T)
            else:
                act(which, core, k * T)


def sum_kernel(gg, gu, gd, md, vd, og, ou, od, mp, vp, own, cor, s1, r1, s2, r2, s3, r3, s4, r4, a1, a2, a3, res, load_sem, ssem, rsem, out_sem, xs, xr, ms, mr):
    at = Place()
    core, bit = at.core, at.bit
    at.greet()
    sems = (ssem, rsem)

    moments = [send(src.at[1 - core], dst, (ms, mr), n, at.peer) for n, (src, dst) in enumerate(((md, mp), (vd, vp)))]
    for copy in moments:
        copy.start()

    def slot(i):
        return lax.rem(i, SLOTS)

    def fetch(i, colour):
        s = slot(i)
        mine, theirs = own.at[colour, s], cor.at[colour, s]
        raw = send(mine, theirs, sems, (0, colour, s), at.peer)
        pl.when(i >= SLOTS)(raw.wait_send)

        def act(which, layer, first):
            if which < 2:
                g = (gg, gu)[which]
                a, b = g.at[layer, :, core, pl.ds(first, T)], g.at[layer, :, 1 - core, pl.ds(first, T)]
            else:
                a, b = gd.at[core, :, pl.ds(first, T)], gd.at[1 - core, :, pl.ds(first, T)]
            send(b, theirs, sems, (0, colour, s), at.peer).start()
            pltpu.make_async_copy(a, mine, load_sem.at[colour, s]).start()

        for_chunk(i, colour, core, act)

    def exchange(stage, i, colour, src, dst):
        s = slot(i)
        return send(src.at[colour, s], dst.at[colour, s], sems, (stage, colour, s), at.partner[ORDER[colour][stage - 1]])

    def block(colour, first_bits, j, free):
        q = 0
        for b, v in zip(ORDER[colour], first_bits):
            q = q + WEIGHT[b] * v
        for n, b in enumerate(ORDER[colour][4 - free :]):
            q = q + WEIGHT[b] * lax.rem(lax.div(j, 2 ** (free - 1 - n)), 2)
        return q

    def f32(ref):
        return ref[...].astype(F32)

    def first(i, colour):
        s = slot(i)
        pltpu.make_async_copy(own.at[colour, s], own.at[colour, s], load_sem.at[colour, s]).wait()
        send(own.at[colour, s], cor.at[colour, s], sems, (0, colour, s), at.peer).wait_recv()
        out = exchange(1, i, colour, s1, r1)
        pl.when(i >= SLOTS)(out.wait_send)
        b1 = ORDER[colour][0]

        def body(j, _):
            q = block(colour, (1 - bit[b1],), j, 3)
            s1[colour, s, j] = (f32(own.at[colour, s, q]) + f32(cor.at[colour, s, q])).astype(BF16)
            return 0

        lax.fori_loop(0, 8, body, 0)
        out.start()

    def second(i, colour):
        s = slot(i)
        exchange(1, i, colour, s1, r1).wait_recv()
        out = exchange(2, i, colour, s2, r2)
        pl.when(i >= SLOTS)(out.wait_send)
        b1, b2 = ORDER[colour][:2]

        def total(j, v):
            q = block(colour, (bit[b1], v), j, 2)
            return f32(own.at[colour, s, q]) + f32(cor.at[colour, s, q]) + f32(r1.at[colour, s, v * 4 + j])

        def give(j, _):
            s2[colour, s, j] = total(j, 1 - bit[b2]).astype(BF16)
            return 0

        def keep(j, _):
            a1[colour, lax.rem(i, 2), j] = total(j, bit[b2])
            return 0

        lax.fori_loop(0, 4, give, 0)
        out.start()
        lax.fori_loop(0, 4, keep, 0)

    def third(i, colour):
        s = slot(i)
        exchange(2, i, colour, s2, r2).wait_recv()
        out = exchange(3, i, colour, s3, r3)
        pl.when(i >= SLOTS)(out.wait_send)
        v = bit[ORDER[colour][2]]

        def give(j, _):
            n = (1 - v) * 2 + j
            s3[colour, s, j] = (a1[colour, lax.rem(i, 2), n] + f32(r2.at[colour, s, n])).astype(BF16)
            return 0

        def keep(j, _):
            n = v * 2 + j
            a2[colour, lax.rem(i, 2), j] = a1[colour, lax.rem(i, 2), n] + f32(r2.at[colour, s, n])
            return 0

        lax.fori_loop(0, 2, give, 0)
        out.start()
        lax.fori_loop(0, 2, keep, 0)

    def fourth(i, colour):
        s = slot(i)
        exchange(3, i, colour, s3, r3).wait_recv()
        out = exchange(4, i, colour, s4, r4)
        pl.when(i >= SLOTS)(out.wait_send)
        v = bit[ORDER[colour][3]]
        s4[colour, s] = (a2[colour, lax.rem(i, 2), 1 - v] + f32(r3.at[colour, s, 1 - v])).astype(BF16)
        out.start()
        a3[colour, lax.rem(i, 2)] = a2[colour, lax.rem(i, 2), v] + f32(r3.at[colour, s, v])

    def result(colour, s, which, layer, first):
        dst = (og, ou, od)[which].at[layer, pl.ds(first, T)]
        return pltpu.make_async_copy(res.at[colour, s], dst, out_sem.at[colour, s])

    def share(i, colour, first):
        return send(res.at[colour, slot(i)], od.at[core, pl.ds(first, T)], (xs, xr), (colour, i - 2 * EACH), at.peer)

    def fifth(i, colour):
        s = slot(i)
        exchange(4, i, colour, s4, r4).wait_recv()
        pl.when(i >= SLOTS)(result(colour, s, 0, 0, 0).wait)

        @pl.when(i >= SLOTS + 2 * EACH)
        def _():
            share(i - SLOTS, colour, 0).wait_send()

        res[colour, s] = (a3[colour, lax.rem(i, 2)] + f32(r4.at[colour, s])).astype(BF16)

        def act(which, layer, first):
            result(colour, s, which, layer, first).start()
            if which == 2:
                share(i, colour, first).start()

        for_chunk(i, colour, core, act)

    for colour in range(2):
        fetch(0, colour)

    def step(i, _):
        @pl.when(i < PAIRS)
        def _():
            for colour in range(2):
                first(i, colour)

        @pl.when(i + 1 < PAIRS)
        def _():
            for colour in range(2):
                fetch(i + 1, colour)

        for late, stage in enumerate((second, third, fourth, fifth), 1):

            @pl.when((i >= late) & (i < PAIRS + late))
            def _():
                for colour in range(2):
                    stage(i - late, colour)

        return 0

    lax.fori_loop(0, PAIRS + 4, step, 0)
    for colour in range(2):
        for s in range(SLOTS):
            send(own.at[colour, s], cor.at[colour, s], sems, (0, colour, s), at.peer).wait_send()
            for stage, (src, dst) in enumerate(((s1, r1), (s2, r2), (s3, r3), (s4, r4)), 1):
                exchange(stage, s, colour, src, dst).wait_send()
            result(colour, s, 0, 0, 0).wait()
            share(PAIRS - SLOTS + s, colour, 0).wait_send()
        for i in range(2 * EACH, PAIRS):
            share(i, colour, 0).wait_recv()
    for copy in moments:
        copy.wait_send()
        copy.wait_recv()


def gather_kernel(wg, wu, wd, og, ou, od, load_sem, ssem, rsem):
    at = Place()
    core, bit, chip = at.core, at.bit, at.chip
    at.greet()
    sems = (ssem, rsem)

    def some(which, layer, first, q):
        return od.at[layer, q, pl.ds(first, T)] if which == 2 else (og, ou)[which].at[layer, q, core, pl.ds(first, T)]

    def mine(which, layer, first):
        return wd.at[pl.ds(first, T)] if which == 2 else (wg, wu)[which].at[layer, pl.ds(first, T)]

    def sized(n, stage, s, colour):
        dst = some(0, 0, 0, pl.ds(0, n))
        return send(dst, dst, sems, (stage, colour, s), at.peer)

    def local(which, layer, first, colour, s):
        return pltpu.make_async_copy(mine(which, layer, first), some(which, layer, first, chip), load_sem.at[colour, s])

    def go(stage, i, colour):
        s = lax.rem(i, SLOTS)
        if stage:
            sized(2 ** (stage - 1), stage - 1, s, colour).wait_recv()
        pl.when(i >= SLOTS)(sized(2**stage, stage, s, colour).wait_send)
        if stage == 1:
            local(0, 0, 0, colour, s).wait()

        def act(which, layer, first):
            if stage == 0:
                local(which, layer, first, colour, s).start()
                send(mine(which, layer, first), some(which, layer, first, chip), sems, (0, colour, s), at.partner[ZH]).start()
            elif stage == 4:
                every = some(which, layer, first, slice(None))
                send(every, every, sems, (4, colour, s), at.peer).start()
            else:
                free = ORDER[colour][4 - stage :]
                for n in range(2**stage):
                    q = chip
                    for m, b in enumerate(free):
                        q = q + WEIGHT[b] * ((n >> m & 1) - bit[b])
                    part = some(which, layer, first, q)
                    send(part, part, sems, (stage, colour, s), at.partner[ORDER[colour][3 - stage]]).start()

        for_chunk(i, colour, core, act)

    def step(i, _):
        for stage in range(5):

            @pl.when((i >= stage) & (i < PAIRS + stage))
            def _():
                for colour in range(2):
                    go(stage, i - stage, colour)

        @pl.when(i >= 5)
        def _():
            for colour in range(2):
                sized(16, 4, lax.rem(i - 5, SLOTS), colour).wait_recv()

        return 0

    lax.fori_loop(0, PAIRS + 5, step, 0)
    for colour in range(2):
        for s in range(SLOTS):
            for stage in range(5):
                sized(2**stage, stage, s, colour).wait_send()


def summed(gg, gu, gd, md, vd):
    any_ = pl.BlockSpec(memory_space=pl.ANY)
    shape = lambda s, d=BF16: jax.ShapeDtypeStruct(s, d)
    vmem = lambda n, k=SLOTS: pltpu.VMEM((2, k, n, T, 8, 128), BF16)
    dma = lambda *s: pltpu.SemaphoreType.DMA(s)
    return pl.pallas_call(
        sum_kernel,
        name="sums",
        out_shape=[shape((2, TILES, 8, 128)), shape((2, TILES, 8, 128)), shape((2, 2 * TILES, 8, 128))] + [shape(md.shape[1:], F32)] * 2,
        in_specs=[any_] * 5,
        out_specs=[any_] * 5,
        scratch_shapes=[
            vmem(16), vmem(16), vmem(8), vmem(8), vmem(4), vmem(4), vmem(2), vmem(2),
            pltpu.VMEM((2, SLOTS, T, 8, 128), BF16), pltpu.VMEM((2, SLOTS, T, 8, 128), BF16),
            pltpu.VMEM((2, 2, 4, T, 8, 128), F32), pltpu.VMEM((2, 2, 2, T, 8, 128), F32), pltpu.VMEM((2, 2, T, 8, 128), F32),
            pltpu.VMEM((2, SLOTS, T, 8, 128), BF16),
            dma(2, SLOTS), dma(5, 2, SLOTS), dma(5, 2, SLOTS), dma(2, SLOTS), dma(2, EACH), dma(2, EACH), dma(2), dma(2),
        ],
        compiler_params=pltpu.CompilerParams(collective_id=0, has_side_effects=True, vmem_limit_bytes=60 * 2**20),
    )(gg, gu, gd, md, vd)


def gathered(wg, wu, wd):
    shape = lambda s: jax.ShapeDtypeStruct(s, BF16)
    dma = lambda *s: pltpu.SemaphoreType.DMA(s)
    return pl.pallas_call(
        gather_kernel,
        name="gather",
        out_shape=[shape((2, 16, 2, TILES, 8, 128))] * 2 + [shape((2, 16, 2 * TILES, 8, 128))],
        in_specs=[pl.BlockSpec(memory_space=pltpu.VMEM)] * 3,
        out_specs=[pl.BlockSpec(memory_space=pl.ANY)] * 3,
        scratch_shapes=[dma(2, SLOTS), dma(5, 2, SLOTS), dma(5, 2, SLOTS)],
        compiler_params=pltpu.CompilerParams(collective_id=1, has_side_effects=True),
    )(wg, wu, wd)


def tiled(a):
    *lead, r, c = a.shape
    n = len(lead)
    a = a.reshape(*lead, r // 8, 8, c // 128, 128)
    return a.swapaxes(n + 1, n + 2).reshape(*lead, r // 8 * (c // 128), 8, 128)


def untiled(a, r, c):
    *lead, _, _, _ = a.shape
    n = len(lead)
    return a.reshape(*lead, r // 8, c // 128, 8, 128).swapaxes(n + 1, n + 2).reshape(*lead, r, c)


def adamw(w, m, v, g):
    m = 0.9 * m + 0.1 * g
    v = 0.95 * v + 0.05 * g * g
    step = m * lax.rsqrt(v + 1e-8) + 0.1 * w
    return (w - 0.02 * step).astype(jnp.bfloat16), m, v


def solution(mesh):
    def step(*arrays):
        terms, weights, m, v = (arrays[i : i + 3] for i in (0, 3, 6, 9))
        me = lax.axis_index("dp")
        chip, core = me // 2, me % 2
        gg, gu = (tiled(t[0]).reshape(2, 16, 2, TILES, 8, 128) for t in terms[:2])
        gd = tiled(terms[2][0]).reshape(2, 16, 2 * TILES, 8, 128)
        sg, su, sd, mp, vp = summed(gg, gu, gd, m[2], v[2])
        new = []
        for n, s in enumerate((sg, su)):
            w = lax.dynamic_slice_in_dim(weights[n], me * 48, 48, 1).astype(F32)
            new.append(adamw(w, m[n], v[n], untiled(s, 48, 4224).astype(F32)))
        sd = untiled(sd, 264, 1536)
        rows = sd.shape[1]
        wd = lax.dynamic_slice_in_dim(weights[2], chip * rows, rows, 1)
        half = rows // 2
        pick = lambda a: lax.dynamic_slice_in_dim(a, core * half, half, 1).astype(F32)
        _, md, vd = adamw(pick(wd), m[2], v[2], pick(sd))
        one = lambda a: lax.dynamic_index_in_dim(a, core, 0, False)
        both = lambda a, p: jnp.where(core == 0, jnp.concatenate([one(a), p]), jnp.concatenate([p, one(a)]))
        nd, _, _ = adamw(one(wd).astype(F32), both(m[2], mp), both(v[2], vp), one(sd).astype(F32))
        og, ou, od = gathered(tiled(new[0][0]), tiled(new[1][0]), tiled(nd))
        whole = [untiled(o.reshape(2, -1, 8, 128), r, c) for o, r, c in ((og, 1536, 4224), (ou, 1536, 4224), (od, 4224, 1536))]
        return (*whole, new[0][1], new[1][1], md, new[0][2], new[1][2], vd)

    all_of, cut = P(None, None, None), P(None, "dp", None)
    return jax.shard_map(
        step,
        mesh=mesh,
        in_specs=(P(("rep", "dp"), None, None, None),) * 3 + (all_of,) * 3 + (cut,) * 6,
        out_specs=(P("rep", None, None),) * 3 + (P("rep", "dp", None),) * 6,
        check_vma=False,
    )
```

```python
import functools

import jax
import jax.numpy as jnp
from jax import lax
from jax.experimental import pallas as pl
from jax.experimental.pallas import tpu as pltpu
from jax.sharding import PartitionSpec as P

MESH = pl.DeviceIdType.MESH
F32, BF16 = jnp.float32, jnp.bfloat16
TILES = 198
T = 9
EACH = TILES // T
PAIRS = 3 * EACH
SLOTS = 4
LIVE = 5
X, Y = range(2)
WEIGHT = (8, 4)
ORDER = ((X, Y), (Y, X))
CORE, FIRST, IN, ACROSS, OUT, LAST, G_LAST, G_IN, G_ACROSS, G_OUT, G_FIRST, G_CORE = range(12)


class Place:
    def __init__(self):
        me = lax.axis_index("dp")
        self.core = lax.rem(me, 2)
        self.chip = lax.div(me, 2)
        self.z = z = lax.rem(self.chip, 4)
        self.bit = (lax.div(me, 16), lax.rem(lax.div(me, 8), 2))
        self.upper = lax.div(z, 2)
        self.lower = 1 - self.upper
        self.inner = lax.rem(z + self.upper, 2) == 1
        self.outer = lax.rem(z + self.upper, 2) == 0
        self.beside = z + 1 - 2 * lax.rem(z, 2)
        self.peer = me + 1 - 2 * self.core
        self.along = tuple(me + 2 * w * (1 - 2 * b) for w, b in zip(WEIGHT, self.bit))
        self.near = me + 2 * (self.beside - z)
        self.far = me + 2 * (3 - 2 * z)

    def greet(self):
        barrier = pltpu.get_barrier_semaphore()
        for other in (self.peer, *self.along, self.near, self.far):
            pl.semaphore_signal(barrier, inc=1, device_id={"dp": other}, device_id_type=MESH)
        pl.semaphore_wait(barrier, 5)


def for_chunk(i, colour, core, act):
    k = 2 * lax.rem(i, EACH) + colour
    for which in range(3):

        @pl.when(lax.div(i, EACH) == which)
        def _():
            if which < 2:
                act(which, lax.div(k, EACH), lax.rem(k, EACH) * T)
            else:
                act(which, core, k * T)


def kernel(
    gg, gu, gd, wg, wu, wd, mg, mu, md, vg, vu, vd, og, ou, od, ng, nu, nd, mx, vx,
    own, cor, s1, r1, s2, r2, s3, r3, s4, r4, s5, r5, acc, mv, wv, res, new,
    load_sem, ssem, rsem, out_sem, local_sem, par_sem, xs, xr, ms, mr,
):
    at = Place()
    core, bit, chip, z = at.core, at.bit, at.chip, at.z
    lower, upper = at.lower, at.upper
    at.greet()

    def send(stage, i, colour, src, dst, device):
        where = (stage, colour, lax.rem(i, SLOTS))
        return pltpu.make_async_remote_copy(
            src_ref=src, dst_ref=dst, send_sem=ssem.at[where], recv_sem=rsem.at[where], device_id={"dp": device}, device_id_type=MESH
        )

    def extra(src, dst, sems, where):
        return pltpu.make_async_remote_copy(
            src_ref=src, dst_ref=dst, send_sem=sems[0].at[where], recv_sem=sems[1].at[where], device_id={"dp": at.peer}, device_id_type=MESH
        )

    moments = [extra(src.at[1 - core], dst, (ms, mr), n) for n, (src, dst) in enumerate(((md, mx), (vd, vx)))]
    for copy in moments:
        copy.start()

    BUFFERS = {CORE: (own, cor), FIRST: (s1, r1), IN: (s2, r2), ACROSS: (s3, r3), OUT: (s4, r4), LAST: (s5, r5)}

    def device(stage, colour):
        b1, b3 = ORDER[colour]
        return {
            CORE: at.peer, FIRST: at.along[b1], IN: at.near, ACROSS: at.far, OUT: at.near, LAST: at.along[b3],
            G_LAST: at.along[b3], G_IN: at.near, G_ACROSS: at.far, G_OUT: at.near, G_FIRST: at.along[b1], G_CORE: at.peer,
        }[stage]

    BLOCKS = {G_LAST: 1, G_IN: 2, G_ACROSS: 4, G_OUT: 6, G_FIRST: 8, G_CORE: 16}

    def some(which, layer, first, q):
        return nd.at[layer, q, pl.ds(first, T)] if which == 2 else (ng, nu)[which].at[layer, q, core, pl.ds(first, T)]

    def whole(stage, i, colour):
        if stage in BUFFERS:
            src, dst = (ref.at[colour, lax.rem(i, SLOTS)] for ref in BUFFERS[stage])
        else:
            src = dst = some(0, 0, 0, pl.ds(0, BLOCKS[stage]))
        return send(stage, i, colour, src, dst, device(stage, colour))

    def free(stage, i, colour):
        pl.when(i >= SLOTS)(whole(stage, i, colour).wait_send)

    def load(i, colour, src):
        s = lax.rem(i, SLOTS)
        return pltpu.make_async_copy(src, own.at[colour, s], load_sem.at[colour, s])

    def fetch(i, colour):
        free(CORE, i, colour)

        def act(which, layer, first):
            if which < 2:
                g = (gg, gu)[which]
                a, b = (g.at[layer, :, c, pl.ds(first, T)] for c in (core, 1 - core))
            else:
                a, b = (gd.at[c, :, pl.ds(first, T)] for c in (core, 1 - core))
            send(CORE, i, colour, b, cor.at[colour, lax.rem(i, SLOTS)], at.peer).start()
            load(i, colour, a).start()

        for_chunk(i, colour, core, act)

    def number(colour, v1, v3, z):
        b1, b3 = ORDER[colour]
        return WEIGHT[b1] * v1 + WEIGHT[b3] * v3 + z

    def f32(ref):
        return ref[...].astype(F32)

    def loop(n, do):
        def one(j, _):
            do(j)
            return 0

        lax.fori_loop(0, n, one, 0)

    def sum_first(i, colour):
        s = lax.rem(i, SLOTS)
        load(i, colour, own.at[colour, s]).wait()
        whole(CORE, i, colour).wait_recv()
        free(FIRST, i, colour)

        def give(j):
            q = number(colour, 1 - bit[ORDER[colour][0]], lax.rem(j, 2), lax.div(j, 2))
            s1[colour, s, j] = (f32(own.at[colour, s, q]) + f32(cor.at[colour, s, q])).astype(BF16)

        loop(8, give)
        whole(FIRST, i, colour).start()

    def sum_in(i, colour):
        s = lax.rem(i, SLOTS)
        whole(FIRST, i, colour).wait_recv()

        def keep(j):
            q = number(colour, bit[ORDER[colour][0]], lax.rem(j, 2), lax.div(j, 2))
            acc[colour, lax.rem(i, LIVE), j] = f32(own.at[colour, s, q]) + f32(cor.at[colour, s, q]) + f32(r1.at[colour, s, j])

        loop(8, keep)

        @pl.when(at.outer)
        def _():
            free(IN, i, colour)

            def give(j):
                s2[colour, s, j] = acc[colour, lax.rem(i, LIVE), lower * 2 + j].astype(BF16)

            loop(6, give)
            whole(IN, i, colour).start()

    def sum_across(i, colour):
        s = lax.rem(i, SLOTS)

        @pl.when(at.inner)
        def _():
            whole(IN, i, colour).wait_recv()
            free(ACROSS, i, colour)

            def give(j):
                s3[colour, s, j] = (acc[colour, lax.rem(i, LIVE), lower * 4 + j] + f32(r2.at[colour, s, lower * 2 + j])).astype(BF16)

            loop(4, give)
            whole(ACROSS, i, colour).start()

            def keep(j):
                acc[colour, lax.rem(i, LIVE), z * 2 + j] += f32(r2.at[colour, s, (z - lower) * 2 + j])

            loop(2, keep)

    def sum_out(i, colour):
        s = lax.rem(i, SLOTS)

        @pl.when(at.inner)
        def _():
            whole(ACROSS, i, colour).wait_recv()
            free(OUT, i, colour)
            there = at.beside

            def give(j):
                s4[colour, s, j] = (acc[colour, lax.rem(i, LIVE), there * 2 + j] + f32(r3.at[colour, s, (there - 2 * upper) * 2 + j])).astype(BF16)

            loop(2, give)
            whole(OUT, i, colour).start()

            def keep(j):
                acc[colour, lax.rem(i, LIVE), z * 2 + j] += f32(r3.at[colour, s, (z - 2 * upper) * 2 + j])

            loop(2, keep)

    def params(i, colour, which, layer, first):
        two = lax.rem(i, 2)
        m, v, w = ((mg, vg, wg), (mu, vu, wu), (md, vd, wd))[which]
        here = pl.ds(first, T)
        pairs = [
            (m.at[layer, here], mv.at[colour, two, 0]),
            (v.at[layer, here], mv.at[colour, two, 1]),
            (w.at[layer, chip, here] if which == 2 else w.at[layer, chip, core, here], wv.at[colour, two]),
        ]
        if which == 2:
            pairs += [(mx.at[here], mv.at[colour, two, 2]), (vx.at[here], mv.at[colour, two, 3])]
        return [pltpu.make_async_copy(src, dst, par_sem.at[colour, two, n]) for n, (src, dst) in enumerate(pairs)]

    def sum_last(i, colour):
        s = lax.rem(i, SLOTS)

        if colour == 0:

            @pl.when(i == 2 * EACH)
            def _():
                for copy in moments:
                    copy.wait_recv()

        def act(*chunk):
            for copy in params(i, colour, *chunk):
                copy.start()

        for_chunk(i, colour, core, act)

        @pl.when(at.outer)
        def _():
            whole(OUT, i, colour).wait_recv()

            def keep(j):
                acc[colour, lax.rem(i, LIVE), z * 2 + j] += f32(r4.at[colour, s, j])

            loop(2, keep)

        free(LAST, i, colour)
        s5[colour, s] = acc[colour, lax.rem(i, LIVE), z * 2 + 1 - bit[ORDER[colour][1]]].astype(BF16)
        whole(LAST, i, colour).start()

    def result(i, colour, which, layer, first):
        s = lax.rem(i, SLOTS)
        return pltpu.make_async_copy(res.at[colour, s], (og, ou, od)[which].at[layer, pl.ds(first, T)], out_sem.at[colour, s])

    def share(i, colour, first):
        return extra(res.at[colour, lax.rem(i, SLOTS)], od.at[core, pl.ds(first, T)], (xs, xr), (colour, i - 2 * EACH))

    def local(i, colour, which, layer, first):
        s = lax.rem(i, SLOTS)
        return pltpu.make_async_copy(new.at[colour, s], some(which, layer, first, chip), local_sem.at[colour, s])

    def update(i, colour):
        s, two = lax.rem(i, SLOTS), lax.rem(i, 2)
        whole(LAST, i, colour).wait_recv()
        pl.when(i >= SLOTS)(result(i, colour, 0, 0, 0).wait)
        pl.when(i >= SLOTS + 2 * EACH)(share(i - SLOTS, colour, 0).wait_send)
        res[colour, s] = (acc[colour, lax.rem(i, LIVE), z * 2 + bit[ORDER[colour][1]]] + f32(r5.at[colour, s])).astype(BF16)
        for copy in params(i, colour, 0, 0, 0):
            copy.wait()

        @pl.when(i >= 2 * EACH)
        def _():
            for copy in params(i, colour, 2, 0, 0)[3:]:
                copy.wait()
            for n in range(2):
                mv[colour, two, n] += mv[colour, two, 2 + n]

        free(G_LAST, i, colour)
        new[colour, s] = adamw(f32(wv.at[colour, two]), mv[colour, two, 0], mv[colour, two, 1], f32(res.at[colour, s]))[0]

        def act(which, layer, first):
            send(G_LAST, i, colour, new.at[colour, s], some(which, layer, first, chip), device(G_LAST, colour)).start()
            local(i, colour, which, layer, first).start()
            result(i, colour, which, layer, first).start()
            if which == 2:
                share(i, colour, first).start()

        for_chunk(i, colour, core, act)

    def units(stage, i, colour, zs):
        free(stage, i, colour)
        v1 = bit[ORDER[colour][0]]

        def act(which, layer, first):
            for there in zs:
                for v3 in range(2):
                    part = some(which, layer, first, number(colour, v1, v3, there))
                    send(stage, i, colour, part, part, device(stage, colour)).start()

        for_chunk(i, colour, core, act)

    def gather_in(i, colour):
        local(i, colour, 0, 0, 0).wait()
        whole(G_LAST, i, colour).wait_recv()
        pl.when(at.outer)(lambda: units(G_IN, i, colour, (z,)))

    def gather_across(i, colour):
        @pl.when(at.inner)
        def _():
            whole(G_IN, i, colour).wait_recv()
            units(G_ACROSS, i, colour, (z, at.beside))

    def gather_out(i, colour):
        @pl.when(at.inner)
        def _():
            whole(G_ACROSS, i, colour).wait_recv()
            units(G_OUT, i, colour, (z, 3 - z, 3 - at.beside))

    def gather_first(i, colour):
        pl.when(at.outer)(whole(G_OUT, i, colour).wait_recv)
        free(G_FIRST, i, colour)

        def act(which, layer, first):
            if ORDER[colour][0] == X:
                parts = [pl.ds(8 * bit[X], 8)]
            else:
                parts = [pl.ds(4 * bit[Y] + 8 * n, 4) for n in range(2)]
            for q in parts:
                part = some(which, layer, first, q)
                send(G_FIRST, i, colour, part, part, device(G_FIRST, colour)).start()

        for_chunk(i, colour, core, act)

    def gather_core(i, colour):
        whole(G_FIRST, i, colour).wait_recv()
        free(G_CORE, i, colour)

        def act(which, layer, first):
            part = some(which, layer, first, slice(None))
            send(G_CORE, i, colour, part, part, at.peer).start()

        for_chunk(i, colour, core, act)

    def gather_done(i, colour):
        whole(G_CORE, i, colour).wait_recv()

    for colour in range(2):
        fetch(0, colour)

    stages = (
        sum_first, None, sum_in, sum_across, sum_out, sum_last, update,
        gather_in, gather_across, gather_out, gather_first, gather_core, gather_done,
    )

    def step(i, _):
        late = 0
        for stage in stages:
            if stage is None:

                @pl.when(i + 1 < PAIRS)
                def _():
                    for colour in range(2):
                        fetch(i + 1, colour)

                continue

            @pl.when((i >= late) & (i < PAIRS + late))
            def _():
                for colour in range(2):
                    stage(i - late, colour)

            late += 1
        return 0

    lax.fori_loop(0, PAIRS + len(stages) - 2, step, 0)
    for colour in range(2):
        for i in range(PAIRS - SLOTS, PAIRS):
            for stage in (CORE, FIRST, LAST, G_LAST, G_FIRST, G_CORE):
                whole(stage, i, colour).wait_send()

            @pl.when(at.outer)
            def _():
                for stage in (IN, G_IN):
                    whole(stage, i, colour).wait_send()

            @pl.when(at.inner)
            def _():
                for stage in (ACROSS, OUT, G_ACROSS, G_OUT):
                    whole(stage, i, colour).wait_send()

            result(i, colour, 0, 0, 0).wait()
            share(i, colour, 0).wait_send()
        for i in range(2 * EACH, PAIRS):
            share(i, colour, 0).wait_recv()
    for copy in moments:
        copy.wait_send()


def fused(*arrays):
    any_ = pl.BlockSpec(memory_space=pl.ANY)
    shape = lambda s, d=BF16: jax.ShapeDtypeStruct(s, d)
    vmem = lambda *n, k=SLOTS, d=BF16: pltpu.VMEM((2, k, *n, T, 8, 128), d)
    dma = lambda *s: pltpu.SemaphoreType.DMA(s)
    sums = [shape((2, n * TILES, 8, 128)) for n in (1, 1, 2)]
    wholes = [shape((2, 16, 2, TILES, 8, 128))] * 2 + [shape((2, 16, 2 * TILES, 8, 128))]
    return pl.pallas_call(
        kernel,
        name="fused",
        out_shape=sums + wholes + [shape((2 * TILES, 8, 128), F32)] * 2,
        in_specs=[any_] * 12,
        out_specs=[any_] * 8,
        scratch_shapes=[
            *(vmem(n) for n in (16, 16, 8, 8, 6, 6, 4, 4, 2, 2)), vmem(), vmem(),
            vmem(8, k=LIVE, d=F32), vmem(4, k=2, d=F32), vmem(k=2), vmem(), vmem(),
            dma(2, SLOTS), dma(12, 2, SLOTS), dma(12, 2, SLOTS), dma(2, SLOTS), dma(2, SLOTS), dma(2, 2, 5),
            dma(2, EACH), dma(2, EACH), dma(2), dma(2),
        ],
        compiler_params=pltpu.CompilerParams(collective_id=0, has_side_effects=True, vmem_limit_bytes=60 * 2**20),
    )(*arrays)


def tiled(a):
    *lead, r, c = a.shape
    n = len(lead)
    a = a.reshape(*lead, r // 8, 8, c // 128, 128)
    return a.swapaxes(n + 1, n + 2).reshape(*lead, r // 8 * (c // 128), 8, 128)


def untiled(a, r, c):
    *lead, _, _, _ = a.shape
    n = len(lead)
    return a.reshape(*lead, r // 8, c // 128, 8, 128).swapaxes(n + 1, n + 2).reshape(*lead, r, c)


def adamw(w, m, v, g):
    m = 0.9 * m + 0.1 * g
    v = 0.95 * v + 0.05 * g * g
    step = m * lax.rsqrt(v + 1e-8) + 0.1 * w
    return (w - 0.02 * step).astype(jnp.bfloat16), m, v


def solution(mesh):
    def step(*arrays):
        terms, weights, m, v = (arrays[i : i + 3] for i in (0, 3, 6, 9))
        core = lax.axis_index("dp") % 2
        half = m[2].shape[1]
        six = lambda a: tiled(a).reshape(2, 16, 2, TILES, 8, 128)
        five = lambda a: tiled(a).reshape(2, 16, 2 * TILES, 8, 128)
        placed = lambda a: tiled(lax.dynamic_update_slice_in_dim(jnp.zeros((2, 2 * half, 1536), F32), a, core * half, 1))
        sg, su, sd, og, ou, od, _, _ = fused(
            six(terms[0][0]), six(terms[1][0]), five(terms[2][0]), six(weights[0]), six(weights[1]), five(weights[2]),
            tiled(m[0]), tiled(m[1]), placed(m[2]), tiled(v[0]), tiled(v[1]), placed(v[2]),
        )
        sd = lax.dynamic_slice_in_dim(untiled(sd, 2 * half, 1536), core * half, half, 1)
        new = []
        for n, g in enumerate((untiled(sg, 48, 4224), untiled(su, 48, 4224), sd)):
            new.append(adamw(jnp.zeros((), F32), m[n], v[n], g.astype(F32))[1:])
        whole = [untiled(o.reshape(2, -1, 8, 128), r, c) for o, r, c in ((og, 1536, 4224), (ou, 1536, 4224), (od, 4224, 1536))]
        return (*whole, *(one[0] for one in new), *(one[1] for one in new))

    all_of, cut = P(None, None, None), P(None, "dp", None)
    return jax.shard_map(
        step,
        mesh=mesh,
        in_specs=(P(("rep", "dp"), None, None, None),) * 3 + (all_of,) * 3 + (cut,) * 6,
        out_specs=(P("rep", None, None),) * 3 + (P("rep", "dp", None),) * 6,
        check_vma=False,
    )
```

```python
import functools

import jax
import jax.numpy as jnp
from jax import lax
from jax.experimental import pallas as pl
from jax.experimental.pallas import tpu as pltpu
from jax.sharding import PartitionSpec as P

MESH = pl.DeviceIdType.MESH
F32, BF16 = jnp.float32, jnp.bfloat16
TILES = 198
T = 6
EACH = TILES // T
PAIRS = 3 * EACH
SLOTS = 4
LIVE = 5
X, Y = range(2)
WEIGHT = (8, 4)
ORDER = ((X, Y), (Y, X))
CORE, FIRST, IN, ACROSS, OUT, LAST, G_LAST, G_IN, G_ACROSS, G_OUT, G_FIRST, G_CORE = range(12)


class Place:
    def __init__(self):
        me = lax.axis_index("dp")
        self.core = lax.rem(me, 2)
        self.chip = lax.div(me, 2)
        self.z = z = lax.rem(self.chip, 4)
        self.bit = (lax.div(me, 16), lax.rem(lax.div(me, 8), 2))
        self.upper = lax.div(z, 2)
        self.lower = 1 - self.upper
        self.inner = lax.rem(z + self.upper, 2) == 1
        self.outer = lax.rem(z + self.upper, 2) == 0
        self.beside = z + 1 - 2 * lax.rem(z, 2)
        self.peer = me + 1 - 2 * self.core
        self.along = tuple(me + 2 * w * (1 - 2 * b) for w, b in zip(WEIGHT, self.bit))
        self.near = me + 2 * (self.beside - z)
        self.far = me + 2 * (3 - 2 * z)

    def greet(self):
        barrier = pltpu.get_barrier_semaphore()
        for other in (self.peer, *self.along, self.near, self.far):
            pl.semaphore_signal(barrier, inc=1, device_id={"dp": other}, device_id_type=MESH)
        pl.semaphore_wait(barrier, 5)


def for_chunk(i, colour, core, act):
    k = 2 * lax.rem(i, EACH) + colour
    for which in range(3):

        @pl.when(lax.div(i, EACH) == which)
        def _():
            if which < 2:
                act(which, lax.div(k, EACH), lax.rem(k, EACH) * T)
            else:
                act(which, core, k * T)


def kernel(
    gg, gu, gd, wg, wu, wd, mg, mu, md, vg, vu, vd, og, ou, od, ng, nu, nd, mx, vx,
    own, cor, s1, r1, s2, r2, s3, r3, s4, r4, s5, r5, acc, mv, wv, res, new,
    load_sem, ssem, rsem, out_sem, local_sem, par_sem, xs, xr, ms, mr,
):
    at = Place()
    core, bit, chip, z = at.core, at.bit, at.chip, at.z
    lower, upper = at.lower, at.upper
    at.greet()

    def send(stage, i, colour, src, dst, device):
        where = (stage, colour, lax.rem(i, SLOTS))
        return pltpu.make_async_remote_copy(
            src_ref=src, dst_ref=dst, send_sem=ssem.at[where], recv_sem=rsem.at[where], device_id={"dp": device}, device_id_type=MESH
        )

    def extra(src, dst, sems, where):
        return pltpu.make_async_remote_copy(
            src_ref=src, dst_ref=dst, send_sem=sems[0].at[where], recv_sem=sems[1].at[where], device_id={"dp": at.peer}, device_id_type=MESH
        )

    moments = [extra(src.at[1 - core], dst, (ms, mr), n) for n, (src, dst) in enumerate(((md, mx), (vd, vx)))]
    for copy in moments:
        copy.start()

    BUFFERS = {CORE: (own, cor), FIRST: (s1, r1), IN: (s2, r2), ACROSS: (s3, r3), OUT: (s4, r4), LAST: (s5, r5)}

    def device(stage, colour):
        b1, b3 = ORDER[colour]
        return {
            CORE: at.peer, FIRST: at.along[b1], IN: at.near, ACROSS: at.far, OUT: at.near, LAST: at.along[b3],
            G_LAST: at.along[b3], G_IN: at.near, G_ACROSS: at.far, G_OUT: at.near, G_FIRST: at.along[b1], G_CORE: at.peer,
        }[stage]

    BLOCKS = {G_LAST: 1, G_IN: 2, G_ACROSS: 4, G_OUT: 6, G_FIRST: 8, G_CORE: 16}

    def some(which, layer, first, q):
        return nd.at[layer, q, pl.ds(first, T)] if which == 2 else (ng, nu)[which].at[layer, q, core, pl.ds(first, T)]

    def whole(stage, i, colour):
        if stage in BUFFERS:
            src, dst = (ref.at[colour, lax.rem(i, SLOTS)] for ref in BUFFERS[stage])
        else:
            src = dst = some(0, 0, 0, pl.ds(0, BLOCKS[stage]))
        return send(stage, i, colour, src, dst, device(stage, colour))

    def free(stage, i, colour):
        pl.when(i >= SLOTS)(whole(stage, i, colour).wait_send)

    def load(i, colour, src):
        s = lax.rem(i, SLOTS)
        return pltpu.make_async_copy(src, own.at[colour, s], load_sem.at[colour, s])

    def fetch(i, colour):
        free(CORE, i, colour)

        def act(which, layer, first):
            if which < 2:
                g = (gg, gu)[which]
                a, b = (g.at[layer, :, c, pl.ds(first, T)] for c in (core, 1 - core))
            else:
                a, b = (gd.at[c, :, pl.ds(first, T)] for c in (core, 1 - core))
            send(CORE, i, colour, b, cor.at[colour, lax.rem(i, SLOTS)], at.peer).start()
            load(i, colour, a).start()

        for_chunk(i, colour, core, act)

    def number(colour, v1, v3, z):
        b1, b3 = ORDER[colour]
        return WEIGHT[b1] * v1 + WEIGHT[b3] * v3 + z

    def f32(ref):
        return ref[...].astype(F32)

    def loop(n, do):
        def one(j, _):
            do(j)
            return 0

        lax.fori_loop(0, n, one, 0)

    def sum_first(i, colour):
        s = lax.rem(i, SLOTS)
        load(i, colour, own.at[colour, s]).wait()
        whole(CORE, i, colour).wait_recv()
        free(FIRST, i, colour)

        def give(j):
            q = number(colour, 1 - bit[ORDER[colour][0]], lax.rem(j, 2), lax.div(j, 2))
            s1[colour, s, j] = (f32(own.at[colour, s, q]) + f32(cor.at[colour, s, q])).astype(BF16)

        loop(8, give)
        whole(FIRST, i, colour).start()

    def sum_in(i, colour):
        s = lax.rem(i, SLOTS)
        whole(FIRST, i, colour).wait_recv()

        def keep(j):
            q = number(colour, bit[ORDER[colour][0]], lax.rem(j, 2), lax.div(j, 2))
            acc[colour, lax.rem(i, LIVE), j] = f32(own.at[colour, s, q]) + f32(cor.at[colour, s, q]) + f32(r1.at[colour, s, j])

        loop(8, keep)

        @pl.when(at.outer)
        def _():
            free(IN, i, colour)

            def give(j):
                s2[colour, s, j] = acc[colour, lax.rem(i, LIVE), lower * 2 + j].astype(BF16)

            loop(6, give)
            whole(IN, i, colour).start()

    def sum_across(i, colour):
        s = lax.rem(i, SLOTS)

        @pl.when(at.inner)
        def _():
            whole(IN, i, colour).wait_recv()
            free(ACROSS, i, colour)

            def give(j):
                s3[colour, s, j] = (acc[colour, lax.rem(i, LIVE), lower * 4 + j] + f32(r2.at[colour, s, lower * 2 + j])).astype(BF16)

            loop(4, give)
            whole(ACROSS, i, colour).start()

            def keep(j):
                acc[colour, lax.rem(i, LIVE), z * 2 + j] += f32(r2.at[colour, s, (z - lower) * 2 + j])

            loop(2, keep)

    def sum_out(i, colour):
        s = lax.rem(i, SLOTS)

        @pl.when(at.inner)
        def _():
            whole(ACROSS, i, colour).wait_recv()
            free(OUT, i, colour)
            there = at.beside

            def give(j):
                s4[colour, s, j] = (acc[colour, lax.rem(i, LIVE), there * 2 + j] + f32(r3.at[colour, s, (there - 2 * upper) * 2 + j])).astype(BF16)

            loop(2, give)
            whole(OUT, i, colour).start()

            def keep(j):
                acc[colour, lax.rem(i, LIVE), z * 2 + j] += f32(r3.at[colour, s, (z - 2 * upper) * 2 + j])

            loop(2, keep)

    def params(i, colour, which, layer, first):
        two = lax.rem(i, 2)
        m, v, w = ((mg, vg, wg), (mu, vu, wu), (md, vd, wd))[which]
        here = pl.ds(first, T)
        pairs = [
            (m.at[layer, here], mv.at[colour, two, 0]),
            (v.at[layer, here], mv.at[colour, two, 1]),
            (w.at[layer, chip, here] if which == 2 else w.at[layer, chip, core, here], wv.at[colour, two]),
        ]
        if which == 2:
            pairs += [(mx.at[here], mv.at[colour, two, 2]), (vx.at[here], mv.at[colour, two, 3])]
        return [pltpu.make_async_copy(src, dst, par_sem.at[colour, two, n]) for n, (src, dst) in enumerate(pairs)]

    def sum_last(i, colour):
        s = lax.rem(i, SLOTS)

        if colour == 0:

            @pl.when(i == 2 * EACH)
            def _():
                for copy in moments:
                    copy.wait_recv()

        def act(*chunk):
            for copy in params(i, colour, *chunk):
                copy.start()

        for_chunk(i, colour, core, act)

        @pl.when(at.outer)
        def _():
            whole(OUT, i, colour).wait_recv()

            def keep(j):
                acc[colour, lax.rem(i, LIVE), z * 2 + j] += f32(r4.at[colour, s, j])

            loop(2, keep)

        free(LAST, i, colour)
        s5[colour, s] = acc[colour, lax.rem(i, LIVE), z * 2 + 1 - bit[ORDER[colour][1]]].astype(BF16)
        whole(LAST, i, colour).start()

    def result(i, colour, which, layer, first):
        s = lax.rem(i, SLOTS)
        return pltpu.make_async_copy(res.at[colour, s], (og, ou, od)[which].at[layer, pl.ds(first, T)], out_sem.at[colour, s])

    def share(i, colour, first):
        return extra(res.at[colour, lax.rem(i, SLOTS)], od.at[core, pl.ds(first, T)], (xs, xr), (colour, i - 2 * EACH))

    def local(i, colour, which, layer, first):
        s = lax.rem(i, SLOTS)
        return pltpu.make_async_copy(new.at[colour, s], some(which, layer, first, chip), local_sem.at[colour, s])

    def update(i, colour):
        s, two = lax.rem(i, SLOTS), lax.rem(i, 2)
        whole(LAST, i, colour).wait_recv()
        pl.when(i >= SLOTS)(result(i, colour, 0, 0, 0).wait)
        pl.when(i >= SLOTS + 2 * EACH)(share(i - SLOTS, colour, 0).wait_send)
        res[colour, s] = (acc[colour, lax.rem(i, LIVE), z * 2 + bit[ORDER[colour][1]]] + f32(r5.at[colour, s])).astype(BF16)
        for copy in params(i, colour, 0, 0, 0):
            copy.wait()

        @pl.when(i >= 2 * EACH)
        def _():
            for copy in params(i, colour, 2, 0, 0)[3:]:
                copy.wait()
            for n in range(2):
                mv[colour, two, n] += mv[colour, two, 2 + n]

        free(G_LAST, i, colour)
        new[colour, s] = adamw(f32(wv.at[colour, two]), mv[colour, two, 0], mv[colour, two, 1], f32(res.at[colour, s]))[0]

        def act(which, layer, first):
            send(G_LAST, i, colour, new.at[colour, s], some(which, layer, first, chip), device(G_LAST, colour)).start()
            local(i, colour, which, layer, first).start()
            result(i, colour, which, layer, first).start()
            if which == 2:
                share(i, colour, first).start()

        for_chunk(i, colour, core, act)

    def units(stage, i, colour, zs):
        free(stage, i, colour)
        v1 = bit[ORDER[colour][0]]

        def act(which, layer, first):
            for there in zs:
                for v3 in range(2):
                    part = some(which, layer, first, number(colour, v1, v3, there))
                    send(stage, i, colour, part, part, device(stage, colour)).start()

        for_chunk(i, colour, core, act)

    def gather_in(i, colour):
        local(i, colour, 0, 0, 0).wait()
        whole(G_LAST, i, colour).wait_recv()
        pl.when(at.outer)(lambda: units(G_IN, i, colour, (z,)))

    def gather_across(i, colour):
        @pl.when(at.inner)
        def _():
            whole(G_IN, i, colour).wait_recv()
            units(G_ACROSS, i, colour, (z, at.beside))

    def gather_out(i, colour):
        @pl.when(at.inner)
        def _():
            whole(G_ACROSS, i, colour).wait_recv()
            units(G_OUT, i, colour, (z, 3 - z, 3 - at.beside))

    def gather_first(i, colour):
        pl.when(at.outer)(whole(G_OUT, i, colour).wait_recv)
        free(G_FIRST, i, colour)

        def act(which, layer, first):
            if ORDER[colour][0] == X:
                parts = [pl.ds(8 * bit[X], 8)]
            else:
                parts = [pl.ds(4 * bit[Y] + 8 * n, 4) for n in range(2)]
            for q in parts:
                part = some(which, layer, first, q)
                send(G_FIRST, i, colour, part, part, device(G_FIRST, colour)).start()

        for_chunk(i, colour, core, act)

    def gather_core(i, colour):
        whole(G_FIRST, i, colour).wait_recv()
        free(G_CORE, i, colour)

        def act(which, layer, first):
            part = some(which, layer, first, slice(None))
            send(G_CORE, i, colour, part, part, at.peer).start()

        for_chunk(i, colour, core, act)

    def gather_done(i, colour):
        whole(G_CORE, i, colour).wait_recv()

    for colour in range(2):
        fetch(0, colour)

    stages = (
        sum_first, None, sum_in, sum_across, sum_out, sum_last, update,
        gather_in, gather_across, gather_out, gather_first, gather_core, gather_done,
    )

    def step(i, _):
        late = 0
        for stage in stages:
            if stage is None:

                @pl.when(i + 1 < PAIRS)
                def _():
                    for colour in range(2):
                        fetch(i + 1, colour)

                continue

            @pl.when((i >= late) & (i < PAIRS + late))
            def _():
                for colour in range(2):
                    stage(i - late, colour)

            late += 1
        return 0

    lax.fori_loop(0, PAIRS + len(stages) - 2, step, 0)
    for colour in range(2):
        for i in range(PAIRS - SLOTS, PAIRS):
            for stage in (CORE, FIRST, LAST, G_LAST, G_FIRST, G_CORE):
                whole(stage, i, colour).wait_send()

            @pl.when(at.outer)
            def _():
                for stage in (IN, G_IN):
                    whole(stage, i, colour).wait_send()

            @pl.when(at.inner)
            def _():
                for stage in (ACROSS, OUT, G_ACROSS, G_OUT):
                    whole(stage, i, colour).wait_send()

            result(i, colour, 0, 0, 0).wait()
            share(i, colour, 0).wait_send()
        for i in range(2 * EACH, PAIRS):
            share(i, colour, 0).wait_recv()
    for copy in moments:
        copy.wait_send()


def fused(*arrays):
    any_ = pl.BlockSpec(memory_space=pl.ANY)
    shape = lambda s, d=BF16: jax.ShapeDtypeStruct(s, d)
    vmem = lambda *n, k=SLOTS, d=BF16: pltpu.VMEM((2, k, *n, T, 8, 128), d)
    dma = lambda *s: pltpu.SemaphoreType.DMA(s)
    sums = [shape((2, n * TILES, 8, 128)) for n in (1, 1, 2)]
    wholes = [shape((2, 16, 2, TILES, 8, 128))] * 2 + [shape((2, 16, 2 * TILES, 8, 128))]
    return pl.pallas_call(
        kernel,
        name="fused",
        out_shape=sums + wholes + [shape((2 * TILES, 8, 128), F32)] * 2,
        in_specs=[any_] * 12,
        out_specs=[any_] * 8,
        scratch_shapes=[
            *(vmem(n) for n in (16, 16, 8, 8, 6, 6, 4, 4, 2, 2)), vmem(), vmem(),
            vmem(8, k=LIVE, d=F32), vmem(4, k=2, d=F32), vmem(k=2), vmem(), vmem(),
            dma(2, SLOTS), dma(12, 2, SLOTS), dma(12, 2, SLOTS), dma(2, SLOTS), dma(2, SLOTS), dma(2, 2, 5),
            dma(2, EACH), dma(2, EACH), dma(2), dma(2),
        ],
        compiler_params=pltpu.CompilerParams(collective_id=0, has_side_effects=True, vmem_limit_bytes=60 * 2**20),
    )(*arrays)


def tiled(a):
    *lead, r, c = a.shape
    n = len(lead)
    a = a.reshape(*lead, r // 8, 8, c // 128, 128)
    return a.swapaxes(n + 1, n + 2).reshape(*lead, r // 8 * (c // 128), 8, 128)


def untiled(a, r, c):
    *lead, _, _, _ = a.shape
    n = len(lead)
    return a.reshape(*lead, r // 8, c // 128, 8, 128).swapaxes(n + 1, n + 2).reshape(*lead, r, c)


def adamw(w, m, v, g):
    m = 0.9 * m + 0.1 * g
    v = 0.95 * v + 0.05 * g * g
    step = m * lax.rsqrt(v + 1e-8) + 0.1 * w
    return (w - 0.02 * step).astype(jnp.bfloat16), m, v


def solution(mesh):
    def step(*arrays):
        terms, weights, m, v = (arrays[i : i + 3] for i in (0, 3, 6, 9))
        core = lax.axis_index("dp") % 2
        half = m[2].shape[1]
        six = lambda a: tiled(a).reshape(2, 16, 2, TILES, 8, 128)
        five = lambda a: tiled(a).reshape(2, 16, 2 * TILES, 8, 128)
        side = lambda a, lo: lax.pad(a, jnp.zeros((), F32), ((0, 0, 0), (lo, half - lo, 0), (0, 0, 0)))
        placed = lambda a: tiled(jnp.where(core == 0, side(a, 0), side(a, half)))
        sg, su, sd, og, ou, od, _, _ = fused(
            six(terms[0][0]), six(terms[1][0]), five(terms[2][0]), six(weights[0]), six(weights[1]), five(weights[2]),
            tiled(m[0]), tiled(m[1]), placed(m[2]), tiled(v[0]), tiled(v[1]), placed(v[2]),
        )
        sd = lax.dynamic_slice_in_dim(untiled(sd, 2 * half, 1536), core * half, half, 1)
        new = []
        for n, g in enumerate((untiled(sg, 48, 4224), untiled(su, 48, 4224), sd)):
            new.append(adamw(jnp.zeros((), F32), m[n], v[n], g.astype(F32))[1:])
        whole = [untiled(o.reshape(2, -1, 8, 128), r, c) for o, r, c in ((og, 1536, 4224), (ou, 1536, 4224), (od, 4224, 1536))]
        return (*whole, *(one[0] for one in new), *(one[1] for one in new))

    all_of, cut = P(None, None, None), P(None, "dp", None)
    return jax.shard_map(
        step,
        mesh=mesh,
        in_specs=(P(("rep", "dp"), None, None, None),) * 3 + (all_of,) * 3 + (cut,) * 6,
        out_specs=(P("rep", None, None),) * 3 + (P("rep", "dp", None),) * 6,
        check_vma=False,
    )
```

```python
import functools

import jax
import jax.numpy as jnp
from jax import lax
from jax.experimental import pallas as pl
from jax.experimental.pallas import tpu as pltpu
from jax.sharding import PartitionSpec as P

MESH = pl.DeviceIdType.MESH
F32, BF16 = jnp.float32, jnp.bfloat16
TILES = 198
T = 6
EACH = TILES // T
PAIRS = 3 * EACH
SLOTS = 4
HELD, EDGE = 204, 192
LIVE = 5
X, Y = range(2)
WEIGHT = (8, 4)
ORDER = ((X, Y), (Y, X))
CORE, FIRST, IN, ACROSS, OUT, LAST, G_LAST, G_IN, G_ACROSS, G_OUT, G_FIRST, G_CORE = range(12)


class Place:
    def __init__(self):
        me = lax.axis_index("dp")
        self.core = lax.rem(me, 2)
        self.chip = lax.div(me, 2)
        self.z = z = lax.rem(self.chip, 4)
        self.bit = (lax.div(me, 16), lax.rem(lax.div(me, 8), 2))
        self.upper = lax.div(z, 2)
        self.lower = 1 - self.upper
        self.inner = lax.rem(z + self.upper, 2) == 1
        self.outer = lax.rem(z + self.upper, 2) == 0
        self.beside = z + 1 - 2 * lax.rem(z, 2)
        self.peer = me + 1 - 2 * self.core
        self.along = tuple(me + 2 * w * (1 - 2 * b) for w, b in zip(WEIGHT, self.bit))
        self.near = me + 2 * (self.beside - z)
        self.far = me + 2 * (3 - 2 * z)

    def greet(self):
        barrier = pltpu.get_barrier_semaphore()
        for other in (self.peer, *self.along, self.near, self.far):
            pl.semaphore_signal(barrier, inc=1, device_id={"dp": other}, device_id_type=MESH)
        pl.semaphore_wait(barrier, 5)


def for_chunk(i, colour, core, act):
    k = 2 * lax.rem(i, EACH) + colour
    for which in range(3):

        @pl.when(lax.div(i, EACH) == which)
        def _():
            if which < 2:
                act(which, lax.div(k, EACH), lax.rem(k, EACH) * T)
            else:
                act(which, core, k * T)


def kernel(
    gg, gu, gd, wg, wu, wd, mg, mu, md, vg, vu, vd, og, ou, od, ng, nu, nd, mx, vx,
    own, cor, s1, r1, s2, r2, s3, r3, s4, r4, s5, r5, acc, mv, wv, res, new,
    load_sem, ssem, rsem, out_sem, local_sem, par_sem, xs, xr, ms, mr,
):
    at = Place()
    core, bit, chip, z = at.core, at.bit, at.chip, at.z
    lower, upper = at.lower, at.upper
    at.greet()

    def send(stage, i, colour, src, dst, device):
        where = (stage, colour, lax.rem(i, SLOTS))
        return pltpu.make_async_remote_copy(
            src_ref=src, dst_ref=dst, send_sem=ssem.at[where], recv_sem=rsem.at[where], device_id={"dp": device}, device_id_type=MESH
        )

    def extra(src, dst, sems, where):
        return pltpu.make_async_remote_copy(
            src_ref=src, dst_ref=dst, send_sem=sems[0].at[where], recv_sem=sems[1].at[where], device_id={"dp": at.peer}, device_id_type=MESH
        )

    moments = [extra(src.at[1 - core], dst, (ms, mr), n) for n, (src, dst) in enumerate(((md, mx), (vd, vx)))]
    for copy in moments:
        copy.start()

    BUFFERS = {CORE: (own, cor), FIRST: (s1, r1), IN: (s2, r2), ACROSS: (s3, r3), OUT: (s4, r4), LAST: (s5, r5)}

    def device(stage, colour):
        b1, b3 = ORDER[colour]
        return {
            CORE: at.peer, FIRST: at.along[b1], IN: at.near, ACROSS: at.far, OUT: at.near, LAST: at.along[b3],
            G_LAST: at.along[b3], G_IN: at.near, G_ACROSS: at.far, G_OUT: at.near, G_FIRST: at.along[b1], G_CORE: at.peer,
        }[stage]

    BLOCKS = {G_LAST: 1, G_IN: 2, G_ACROSS: 4, G_OUT: 6, G_FIRST: 8, G_CORE: 16}

    def some(which, layer, first, q):
        return nd.at[layer, q, pl.ds(first, T)] if which == 2 else (ng, nu)[which].at[layer, q, core, pl.ds(first, T)]

    def whole(stage, i, colour):
        if stage in BUFFERS:
            src, dst = (ref.at[colour, lax.rem(i, SLOTS)] for ref in BUFFERS[stage])
        else:
            src = dst = some(0, 0, 0, pl.ds(0, BLOCKS[stage]))
        return send(stage, i, colour, src, dst, device(stage, colour))

    def free(stage, i, colour):
        pl.when(i >= SLOTS)(whole(stage, i, colour).wait_send)

    def load(i, colour, src):
        s = lax.rem(i, SLOTS)
        return pltpu.make_async_copy(src, own.at[colour, s], load_sem.at[colour, s])

    def fetch(i, colour):
        free(CORE, i, colour)

        def act(which, layer, first):
            if which < 2:
                g = (gg, gu)[which]
                a, b = (g.at[layer, :, c, pl.ds(first, T)] for c in (core, 1 - core))
            else:
                a, b = (gd.at[c, :, pl.ds(first, T)] for c in (core, 1 - core))
            send(CORE, i, colour, b, cor.at[colour, lax.rem(i, SLOTS)], at.peer).start()
            load(i, colour, a).start()

        for_chunk(i, colour, core, act)

    def number(colour, v1, v3, z):
        b1, b3 = ORDER[colour]
        return WEIGHT[b1] * v1 + WEIGHT[b3] * v3 + z

    def f32(ref):
        return ref[...].astype(F32)

    def loop(n, do):
        def one(j, _):
            do(j)
            return 0

        lax.fori_loop(0, n, one, 0)

    def sum_first(i, colour):
        s = lax.rem(i, SLOTS)
        load(i, colour, own.at[colour, s]).wait()
        whole(CORE, i, colour).wait_recv()
        free(FIRST, i, colour)

        def give(j):
            q = number(colour, 1 - bit[ORDER[colour][0]], lax.rem(j, 2), lax.div(j, 2))
            s1[colour, s, j] = (f32(own.at[colour, s, q]) + f32(cor.at[colour, s, q])).astype(BF16)

        loop(8, give)
        whole(FIRST, i, colour).start()

    def sum_in(i, colour):
        s = lax.rem(i, SLOTS)
        whole(FIRST, i, colour).wait_recv()

        def keep(j):
            q = number(colour, bit[ORDER[colour][0]], lax.rem(j, 2), lax.div(j, 2))
            acc[colour, lax.rem(i, LIVE), j] = f32(own.at[colour, s, q]) + f32(cor.at[colour, s, q]) + f32(r1.at[colour, s, j])

        loop(8, keep)

        @pl.when(at.outer)
        def _():
            free(IN, i, colour)

            def give(j):
                s2[colour, s, j] = acc[colour, lax.rem(i, LIVE), lower * 2 + j].astype(BF16)

            loop(6, give)
            whole(IN, i, colour).start()

    def sum_across(i, colour):
        s = lax.rem(i, SLOTS)

        @pl.when(at.inner)
        def _():
            whole(IN, i, colour).wait_recv()
            free(ACROSS, i, colour)

            def give(j):
                s3[colour, s, j] = (acc[colour, lax.rem(i, LIVE), lower * 4 + j] + f32(r2.at[colour, s, lower * 2 + j])).astype(BF16)

            loop(4, give)
            whole(ACROSS, i, colour).start()

            def keep(j):
                acc[colour, lax.rem(i, LIVE), z * 2 + j] += f32(r2.at[colour, s, (z - lower) * 2 + j])

            loop(2, keep)

    def sum_out(i, colour):
        s = lax.rem(i, SLOTS)

        @pl.when(at.inner)
        def _():
            whole(ACROSS, i, colour).wait_recv()
            free(OUT, i, colour)
            there = at.beside

            def give(j):
                s4[colour, s, j] = (acc[colour, lax.rem(i, LIVE), there * 2 + j] + f32(r3.at[colour, s, (there - 2 * upper) * 2 + j])).astype(BF16)

            loop(2, give)
            whole(OUT, i, colour).start()

            def keep(j):
                acc[colour, lax.rem(i, LIVE), z * 2 + j] += f32(r3.at[colour, s, (z - 2 * upper) * 2 + j])

            loop(2, keep)

    def params(i, colour, which, layer, first):
        two = lax.rem(i, 2)
        here = pl.ds(first, T)

        def copies(*pairs):
            return [pltpu.make_async_copy(src, dst, par_sem.at[colour, two, n]) for n, src, dst in pairs]

        def both(m, v, n, sem):
            return copies((sem, m, mv.at[colour, two, n]), (sem + 1, v, mv.at[colour, two, n + 1]))

        w = (wg, wu, wd)[which]
        weight = copies((2, w.at[layer, chip, here] if which == 2 else w.at[layer, chip, core, here], wv.at[colour, two]))
        if which < 2:
            m, v = ((mg, vg), (mu, vu))[which]
            return weight + both(m.at[layer, here], v.at[layer, here], 0, 0), [], []
        ours, theirs = pl.ds(first - EDGE * core, T), pl.ds(first - EDGE * (1 - core), T)
        return (
            weight + both(md.at[core, ours], vd.at[core, ours], 0, 0),
            both(mx.at[theirs], vx.at[theirs], 0, 0),
            both(mx.at[theirs], vx.at[theirs], 2, 3),
        )

    def sum_last(i, colour):
        s = lax.rem(i, SLOTS)

        if colour == 0:

            @pl.when(i == 2 * EACH)
            def _():
                for copy in moments:
                    copy.wait_recv()

        def act(*chunk):
            here, there, edge = params(i, colour, *chunk)
            if not edge:
                for copy in here:
                    copy.start()
                return
            first = chunk[2]
            here[0].start()
            mine = ((core == 0) & (first < HELD)) | ((core == 1) & (first >= EDGE))
            for condition, some_ in ((mine, here[1:]), (~mine, there), ((first >= EDGE) & (first < HELD), edge)):

                @pl.when(condition)
                def _():
                    for copy in some_:
                        copy.start()

        for_chunk(i, colour, core, act)

        @pl.when(at.outer)
        def _():
            whole(OUT, i, colour).wait_recv()

            def keep(j):
                acc[colour, lax.rem(i, LIVE), z * 2 + j] += f32(r4.at[colour, s, j])

            loop(2, keep)

        free(LAST, i, colour)
        s5[colour, s] = acc[colour, lax.rem(i, LIVE), z * 2 + 1 - bit[ORDER[colour][1]]].astype(BF16)
        whole(LAST, i, colour).start()

    def result(i, colour, which, layer, first):
        s = lax.rem(i, SLOTS)
        return pltpu.make_async_copy(res.at[colour, s], (og, ou, od)[which].at[layer, pl.ds(first, T)], out_sem.at[colour, s])

    def share(i, colour, first):
        return extra(res.at[colour, lax.rem(i, SLOTS)], od.at[core, pl.ds(first, T)], (xs, xr), (colour, i - 2 * EACH))

    def local(i, colour, which, layer, first):
        s = lax.rem(i, SLOTS)
        return pltpu.make_async_copy(new.at[colour, s], some(which, layer, first, chip), local_sem.at[colour, s])

    def update(i, colour):
        s, two = lax.rem(i, SLOTS), lax.rem(i, 2)
        whole(LAST, i, colour).wait_recv()
        pl.when(i >= SLOTS)(result(i, colour, 0, 0, 0).wait)
        pl.when(i >= SLOTS + 2 * EACH)(share(i - SLOTS, colour, 0).wait_send)
        res[colour, s] = (acc[colour, lax.rem(i, LIVE), z * 2 + bit[ORDER[colour][1]]] + f32(r5.at[colour, s])).astype(BF16)
        for copy in params(i, colour, 0, 0, 0)[0]:
            copy.wait()
        first = (2 * lax.rem(i, EACH) + colour) * T

        @pl.when((i >= 2 * EACH) & (first >= EDGE) & (first < HELD))
        def _():
            for n in range(2):
                pltpu.make_async_copy(mv.at[colour, two, n], mv.at[colour, two, 2 + n], par_sem.at[colour, two, 3 + n]).wait()
            for n in range(2):
                mv[colour, two, n] += mv[colour, two, 2 + n]

        free(G_LAST, i, colour)
        new[colour, s] = adamw(f32(wv.at[colour, two]), mv[colour, two, 0], mv[colour, two, 1], f32(res.at[colour, s]))[0]

        def act(which, layer, first):
            send(G_LAST, i, colour, new.at[colour, s], some(which, layer, first, chip), device(G_LAST, colour)).start()
            local(i, colour, which, layer, first).start()
            result(i, colour, which, layer, first).start()
            if which == 2:
                share(i, colour, first).start()

        for_chunk(i, colour, core, act)

    def units(stage, i, colour, zs):
        free(stage, i, colour)
        v1 = bit[ORDER[colour][0]]

        def act(which, layer, first):
            for there in zs:
                for v3 in range(2):
                    part = some(which, layer, first, number(colour, v1, v3, there))
                    send(stage, i, colour, part, part, device(stage, colour)).start()

        for_chunk(i, colour, core, act)

    def gather_in(i, colour):
        local(i, colour, 0, 0, 0).wait()
        whole(G_LAST, i, colour).wait_recv()
        pl.when(at.outer)(lambda: units(G_IN, i, colour, (z,)))

    def gather_across(i, colour):
        @pl.when(at.inner)
        def _():
            whole(G_IN, i, colour).wait_recv()
            units(G_ACROSS, i, colour, (z, at.beside))

    def gather_out(i, colour):
        @pl.when(at.inner)
        def _():
            whole(G_ACROSS, i, colour).wait_recv()
            units(G_OUT, i, colour, (z, 3 - z, 3 - at.beside))

    def gather_first(i, colour):
        pl.when(at.outer)(whole(G_OUT, i, colour).wait_recv)
        free(G_FIRST, i, colour)

        def act(which, layer, first):
            if ORDER[colour][0] == X:
                parts = [pl.ds(8 * bit[X], 8)]
            else:
                parts = [pl.ds(4 * bit[Y] + 8 * n, 4) for n in range(2)]
            for q in parts:
                part = some(which, layer, first, q)
                send(G_FIRST, i, colour, part, part, device(G_FIRST, colour)).start()

        for_chunk(i, colour, core, act)

    def gather_core(i, colour):
        whole(G_FIRST, i, colour).wait_recv()
        free(G_CORE, i, colour)

        def act(which, layer, first):
            part = some(which, layer, first, slice(None))
            send(G_CORE, i, colour, part, part, at.peer).start()

        for_chunk(i, colour, core, act)

    def gather_done(i, colour):
        whole(G_CORE, i, colour).wait_recv()

    for colour in range(2):
        fetch(0, colour)

    stages = (
        sum_first, None, sum_in, sum_across, sum_out, sum_last, update,
        gather_in, gather_across, gather_out, gather_first, gather_core, gather_done,
    )

    def step(i, _):
        late = 0
        for stage in stages:
            if stage is None:

                @pl.when(i + 1 < PAIRS)
                def _():
                    for colour in range(2):
                        fetch(i + 1, colour)

                continue

            @pl.when((i >= late) & (i < PAIRS + late))
            def _():
                for colour in range(2):
                    stage(i - late, colour)

            late += 1
        return 0

    lax.fori_loop(0, PAIRS + len(stages) - 2, step, 0)
    for colour in range(2):
        for i in range(PAIRS - SLOTS, PAIRS):
            for stage in (CORE, FIRST, LAST, G_LAST, G_FIRST, G_CORE):
                whole(stage, i, colour).wait_send()

            @pl.when(at.outer)
            def _():
                for stage in (IN, G_IN):
                    whole(stage, i, colour).wait_send()

            @pl.when(at.inner)
            def _():
                for stage in (ACROSS, OUT, G_ACROSS, G_OUT):
                    whole(stage, i, colour).wait_send()

            result(i, colour, 0, 0, 0).wait()
            share(i, colour, 0).wait_send()
        for i in range(2 * EACH, PAIRS):
            share(i, colour, 0).wait_recv()
    for copy in moments:
        copy.wait_send()


def fused(*arrays):
    any_ = pl.BlockSpec(memory_space=pl.ANY)
    shape = lambda s, d=BF16: jax.ShapeDtypeStruct(s, d)
    vmem = lambda *n, k=SLOTS, d=BF16: pltpu.VMEM((2, k, *n, T, 8, 128), d)
    dma = lambda *s: pltpu.SemaphoreType.DMA(s)
    sums = [shape((2, n * TILES, 8, 128)) for n in (1, 1, 2)]
    wholes = [shape((2, 16, 2, TILES, 8, 128))] * 2 + [shape((2, 16, 2 * TILES, 8, 128))]
    return pl.pallas_call(
        kernel,
        name="fused",
        out_shape=sums + wholes + [shape((HELD, 8, 128), F32)] * 2,
        in_specs=[any_] * 12,
        out_specs=[any_] * 8,
        scratch_shapes=[
            *(vmem(n) for n in (16, 16, 8, 8, 6, 6, 4, 4, 2, 2)), vmem(), vmem(),
            vmem(8, k=LIVE, d=F32), vmem(4, k=2, d=F32), vmem(k=2), vmem(), vmem(),
            dma(2, SLOTS), dma(12, 2, SLOTS), dma(12, 2, SLOTS), dma(2, SLOTS), dma(2, SLOTS), dma(2, 2, 5),
            dma(2, EACH), dma(2, EACH), dma(2), dma(2),
        ],
        compiler_params=pltpu.CompilerParams(collective_id=0, has_side_effects=True, vmem_limit_bytes=60 * 2**20),
    )(*arrays)


def tiled(a):
    *lead, r, c = a.shape
    n = len(lead)
    a = a.reshape(*lead, r // 8, 8, c // 128, 128)
    return a.swapaxes(n + 1, n + 2).reshape(*lead, r // 8 * (c // 128), 8, 128)


def untiled(a, r, c):
    *lead, _, _, _ = a.shape
    n = len(lead)
    return a.reshape(*lead, r // 8, c // 128, 8, 128).swapaxes(n + 1, n + 2).reshape(*lead, r, c)


def adamw(w, m, v, g):
    m = 0.9 * m + 0.1 * g
    v = 0.95 * v + 0.05 * g * g
    step = m * lax.rsqrt(v + 1e-8) + 0.1 * w
    return (w - 0.02 * step).astype(jnp.bfloat16), m, v


def solution(mesh):
    def step(*arrays):
        terms, weights, m, v = (arrays[i : i + 3] for i in (0, 3, 6, 9))
        core = lax.axis_index("dp") % 2
        half = m[2].shape[1]
        six = lambda a: tiled(a).reshape(2, 16, 2, TILES, 8, 128)
        five = lambda a: tiled(a).reshape(2, 16, 2 * TILES, 8, 128)
        side = lambda a, lo: lax.pad(a, jnp.zeros((), F32), ((0, 0, 0), (lo, -half % 8 - lo, 0), (0, 0, 0)))
        placed = lambda a: tiled(jnp.where(core == 0, side(a, 0), side(a, -half % 8)))
        sg, su, sd, og, ou, od, _, _ = fused(
            six(terms[0][0]), six(terms[1][0]), five(terms[2][0]), six(weights[0]), six(weights[1]), five(weights[2]),
            tiled(m[0]), tiled(m[1]), placed(m[2]), tiled(v[0]), tiled(v[1]), placed(v[2]),
        )
        sd = lax.dynamic_slice_in_dim(untiled(sd, 2 * half, 1536), core * half, half, 1)
        new = []
        for n, g in enumerate((untiled(sg, 48, 4224), untiled(su, 48, 4224), sd)):
            new.append(adamw(jnp.zeros((), F32), m[n], v[n], g.astype(F32))[1:])
        whole = [untiled(o.reshape(2, -1, 8, 128), r, c) for o, r, c in ((og, 1536, 4224), (ou, 1536, 4224), (od, 4224, 1536))]
        return (*whole, *(one[0] for one in new), *(one[1] for one in new))

    all_of, cut = P(None, None, None), P(None, "dp", None)
    return jax.shard_map(
        step,
        mesh=mesh,
        in_specs=(P(("rep", "dp"), None, None, None),) * 3 + (all_of,) * 3 + (cut,) * 6,
        out_specs=(P("rep", None, None),) * 3 + (P("rep", "dp", None),) * 6,
        check_vma=False,
    )
```
